32 devices in a mesh: prompt: 4 (over y, x), sample: 8 (over z, core).
Axes of the slice: x: 2, y: 2, z: 4, core: 2. Of those that a mesh axis runs over, the one named last changes fastest.
Arguments:
- queries: bfloat16 [4, 64, 4096], P('prompt', 'sample'), may hold values from -250 to 250
- prompt_cache: bfloat16 [4, 8, 2048, 2048], P('prompt', 'sample'), may hold values from -6 to 6
- owner: int32 [4], P('prompt'), may hold values from 0 to 7
- prompt_len: int32 [4], P('prompt'), may hold values from 512 to 2048
- suffix_cache: bfloat16 [4, 64, 256, 2048], P('prompt', 'sample'), may hold values from -6 to 6
- suffix_len: int32 [4, 64], P('prompt', 'sample'), may hold values from 1 to 256
- new_kv: bfloat16 [4, 64, 2048], P('prompt', 'sample'), may hold values from -6 to 6
- out_weight: bfloat16 [4096, 4096], P(None, 'sample'), may hold values from -0.09375 to 0.09375
Outputs:
- mixed: bfloat16 [4, 64, 4096], P('prompt', None, 'sample')
The draws below stay inside these ranges and needn't reach their ends.
All inputs are finite; a program needn't handle non-finite values.
Results may differ from the reference program's by a relative error of at most 0.007.
Values may be sent and summed in bfloat16 or wider, within the bound.
A program may use at most 192 MiB of HBM per device.

```python
import jax
import jax.numpy as jnp
from jax import lax

D = 4096
H = 32
KVH = 8
HD = 128
PLEN = 2048
SLEN = 256
PROMPTS = 4
SLOTS = 8
SAMPLES = 64
QW = 4096
KV2 = 2048
N_SAMPLE = 8


def shared_draw(key):
    key_cache, key_query = jax.random.split(jax.random.fold_in(key, 7))
    cache = jnp.clip(jax.random.normal(key_cache, (PROMPTS, SLOTS, PLEN, KV2), jnp.float32), -6.0, 6.0)
    queries = 0.5 * jnp.clip(jax.random.normal(key_query, (PROMPTS, SAMPLES, H * HD), jnp.float32), -6.0, 6.0)
    return (cache, queries)


def draw_queries(key, part):
    return shared_draw(key)[1].astype(jnp.bfloat16)


def draw_prompt_cache(key, part):
    return shared_draw(key)[0].astype(jnp.bfloat16)


def with_ends(values, rng, smallest, high):
    shape = values.shape
    spot = [jax.random.randint(jax.random.fold_in(rng, axis), (), 0, shape[axis]) for axis in range(len(shape))]
    values = values.at[tuple(spot)].set(smallest)
    longest = shape.index(max(shape))
    spot[longest] = (spot[longest] + 1) % shape[longest]
    return values.at[tuple(spot)].set(high)


def shard_levels(key, shape, cuts, smallest, largest):
    gain = 1.0
    for dim, blocks in cuts:
        steps = jax.random.uniform(jax.random.fold_in(jax.random.fold_in(key, 6), dim), (blocks,), jnp.float32, smallest / len(cuts), largest / len(cuts))
        gain = gain * jnp.repeat(jnp.exp(steps), shape[dim] // blocks).reshape((-1,) + (1,) * (len(shape) - 1 - dim))
    return gain


def noise(rng, shape, deviation, reach, cuts=(), kind=jnp.bfloat16):
    result = deviation * jax.random.normal(rng, shape, jnp.float32)
    if cuts:
        result = result * shard_levels(rng, shape, cuts, -0.22, 0.18)
    return jnp.clip(result, -reach, reach).astype(kind)


def setup_inputs(seed: int = 0) -> dict:
    streams_of = jax.random.split(jax.random.key(seed), 9)
    queries = draw_queries(jax.random.fold_in(streams_of[8], 71), 0)
    prompt_cache = draw_prompt_cache(jax.random.fold_in(streams_of[8], 71), 0)
    owner = with_ends(jax.random.randint(streams_of[2], (PROMPTS,), 0, N_SAMPLE), jax.random.fold_in(streams_of[2], 1), 0, N_SAMPLE - 1).astype(jnp.int32)
    prompt_len = with_ends(jax.random.randint(streams_of[3], (PROMPTS,), PLEN // 4, PLEN + 1), jax.random.fold_in(streams_of[3], 1), PLEN // 4, PLEN).astype(jnp.int32)
    suffix_cache = noise(streams_of[4], (PROMPTS, SAMPLES, SLEN, KV2), 1.0, 6.0, ((0, 4), (1, 8)))
    suffix_len = with_ends(jax.random.randint(streams_of[5], (PROMPTS, SAMPLES), 1, SLEN + 1), jax.random.fold_in(streams_of[5], 1), 1, SLEN).astype(jnp.int32)
    new_kv = noise(streams_of[6], (PROMPTS, SAMPLES, KV2), 1.0, 6.0, ((0, 4), (1, 8)))
    out_weight = noise(streams_of[7], (QW, D), QW ** -0.5, 0.09375, ((1, 8),))
    return {"queries": queries, "prompt_cache": prompt_cache, "owner": owner, "prompt_len": prompt_len, "suffix_cache": suffix_cache, "suffix_len": suffix_len, "new_kv": new_kv, "out_weight": out_weight}


def prefix_part(queries, cache, length):
    count = queries.shape[0]
    positions = cache.shape[0]
    query = queries.astype(jnp.float32).reshape(count, KVH, H // KVH, HD)
    keys = cache[:, :KVH * HD].astype(jnp.float32).reshape(positions, KVH, HD)
    values = cache[:, KVH * HD:].astype(jnp.float32).reshape(positions, KVH, HD)
    scores = jnp.einsum("sgjd,tgd->sgjt", query, keys) * (HD ** -0.5)
    valid = jnp.arange(positions, dtype=jnp.int32) < length
    scores = jnp.where(valid, scores, -1e30)
    top = jnp.max(scores, axis=-1)
    weights = jnp.exp(scores - top[..., None])
    total = jnp.sum(weights, axis=-1)
    rounded = weights.astype(jnp.bfloat16).astype(jnp.float32)
    output = jnp.einsum("sgjt,tgd->sgjd", rounded, values)
    return output.reshape(count, H, HD), top.reshape(count, H), total.reshape(count, H)


def suffix_part(queries, cache, lengths, own):
    count = queries.shape[0]
    positions = cache.shape[1]
    query = queries.astype(jnp.float32).reshape(count, KVH, H // KVH, HD)
    keys = cache[:, :, :KVH * HD].astype(jnp.float32).reshape(count, positions, KVH, HD)
    values = cache[:, :, KVH * HD:].astype(jnp.float32).reshape(count, positions, KVH, HD)
    own_key = own[:, :KVH * HD].astype(jnp.float32).reshape(count, KVH, HD)
    own_value = own[:, KVH * HD:].astype(jnp.float32).reshape(count, KVH, HD)
    scores = jnp.einsum("sgjd,stgd->sgjt", query, keys) * (HD ** -0.5)
    valid = jnp.arange(positions, dtype=jnp.int32)[None, :] < lengths[:, None]
    scores = jnp.where(valid[:, None, None, :], scores, -1e30)
    own_score = jnp.einsum("sgjd,sgd->sgj", query, own_key) * (HD ** -0.5)
    top = jnp.maximum(jnp.max(scores, axis=-1), own_score)
    weights = jnp.exp(scores - top[..., None])
    own_weight = jnp.exp(own_score - top)
    total = jnp.sum(weights, axis=-1) + own_weight
    rounded = weights.astype(jnp.bfloat16).astype(jnp.float32)
    output = jnp.einsum("sgjt,stgd->sgjd", rounded, values)
    own_rounded = own_weight.astype(jnp.bfloat16).astype(jnp.float32)
    output = output + own_rounded[..., None] * own_value[:, :, None, :]
    return output.reshape(count, H, HD), top.reshape(count, H), total.reshape(count, H)


def combine(prefix, suffix):
    out_pre, top_pre, total_pre = prefix
    out_suf, top_suf, total_suf = suffix
    top = jnp.maximum(top_pre, top_suf)
    factor_pre = jnp.exp(top_pre - top)
    factor_suf = jnp.exp(top_suf - top)
    numer = out_pre * factor_pre[..., None] + out_suf * factor_suf[..., None]
    denom = total_pre * factor_pre + total_suf * factor_suf
    attn = numer / denom[..., None]
    return attn.reshape(attn.shape[0], H * HD).astype(jnp.bfloat16)


def reference(queries, prompt_cache, owner, prompt_len, suffix_cache, suffix_len, new_kv, out_weight):
    def one_prompt(index):
        prefix = prefix_part(queries[index], prompt_cache[index, owner[index]], prompt_len[index])
        suffix = suffix_part(queries[index], suffix_cache[index], suffix_len[index], new_kv[index])
        attn = combine(prefix, suffix)
        return jnp.dot(attn, out_weight, preferred_element_type=jnp.float32).astype(jnp.bfloat16)

    return lax.map(one_prompt, jnp.arange(PROMPTS, dtype=jnp.int32))
```

```python
import functools

import jax
import jax.numpy as jnp
from jax import lax
from jax.experimental import pallas as pl
from jax.experimental.pallas import tpu as pltpu
from jax.sharding import PartitionSpec as P

H = 32
KVH = 8
HD = 128
GROUP = H // KVH
HALF_H = H // 2
HALF_G = KVH // 2
HALF_W = HALF_H * HD
KW = KVH * HD
GW = GROUP * HD
FACTOR = HD ** (-0.5) * 1.4426950408889634
NEG = -1e30
F32 = jnp.float32
BF16 = jnp.bfloat16
NT = (((1,), (1,)), ((), ()))


def kernel(
    n,
    owner_ref,
    plen_ref,
    slen_ref,
    q_ref,
    new_ref,
    cache_ref,
    suffix_ref,
    w_ref,
    out_ref,
    kv0,
    kv1,
    kv2,
    kv3,
    suf,
    wbuf,
    qsrc,
    qall,
    qrow,
    orow,
    ssrc,
    sall,
    stsrc,
    stall,
    mine,
    minest,
    from_left,
    from_left_st,
    from_right,
    from_right_st,
    to_right,
    to_right_st,
    to_left,
    to_left_st,
    attn,
    attn_in,
    suf_sem,
    kv_sem,
    w_sem,
    q_sem,
    q_send,
    q_recv,
    s_send,
    s_recv,
    t_send,
    t_recv,
    kv_send,
    kv_recv,
    r_send,
    r_recv,
    l_send,
    l_recv,
    a_send,
    a_recv,
):
    kv = (kv0, kv1, kv2, kv3)
    me = lax.axis_index("sample")
    chip = me // 2
    core = me % 2
    chips = n // 2
    partner = chip * 2 + (1 - core)
    count = q_ref.shape[1]
    total = n * count
    slen = suffix_ref.shape[2]

    def remote(src, dst, send, recv, to):
        return pltpu.make_async_remote_copy(
            src_ref=src,
            dst_ref=dst,
            send_sem=send,
            recv_sem=recv,
            device_id={"sample": to},
            device_id_type=pl.DeviceIdType.MESH,
        )

    suf_copies = [
        pltpu.make_async_copy(suffix_ref.at[0, b], suf.at[b], suf_sem.at[b])
        for b in range(count)
    ]
    for copy in suf_copies:
        copy.start()

    barrier = pltpu.get_barrier_semaphore()
    for d in range(1, n):
        pl.semaphore_signal(
            barrier,
            inc=1,
            device_id={"sample": (me + d) % n},
            device_id_type=pl.DeviceIdType.MESH,
        )

    q32 = q_ref[0].astype(F32)
    for half in range(2):
        qsrc[half] = q_ref[0, :, half * HALF_W : (half + 1) * HALF_W]
    for h in range(H):
        qrow[h * count : (h + 1) * count, :] = q32[:, h * HD : (h + 1) * HD]

    def kv_local(k, part):
        col = part * KW + (core * HALF_G + k) * HD
        return pltpu.make_async_copy(
            cache_ref.at[0, 0, :, pl.ds(pl.multiple_of(col, HD), HD)],
            kv[k].at[core, part],
            kv_sem.at[k, part],
        )

    def kv_remote(k, part):
        col = part * KW + ((1 - core) * HALF_G + k) * HD
        return remote(
            cache_ref.at[0, 0, :, pl.ds(pl.multiple_of(col, HD), HD)],
            kv[k].at[core, part],
            kv_send.at[k, part],
            kv_recv.at[k, part],
            partner,
        )

    def kv_arrival(k, part):
        return remote(
            kv[k].at[1 - core, part],
            kv[k].at[1 - core, part],
            kv_send.at[k, part],
            kv_recv.at[k, part],
            partner,
        )

    def w_copy(half):
        return pltpu.make_async_copy(
            w_ref.at[pl.ds(half * HALF_W, HALF_W), :], wbuf.at[half], w_sem.at[half]
        )

    pl.semaphore_wait(barrier, n - 1)

    def q_copy(d):
        to = (me + d) % n
        return remote(qsrc.at[to % 2], qall.at[me], q_send.at[d], q_recv.at[d], to)

    order = sorted(range(1, n), key=lambda d: -min(d, n - d))
    for d in order:
        q_copy(d).start()
    own_q = pltpu.make_async_copy(qsrc.at[core], qall.at[me], q_sem)
    own_q.start()
    for k in range(HALF_G):
        for part in range(2):
            kv_remote(k, part).start()
    for k in range(HALF_G):
        for part in range(2):
            kv_local(k, part).start()
    for half in range(2):
        w_copy(half).start()

    row_group = lax.broadcasted_iota(jnp.int32, (H, HD), 0) // GROUP
    lane = lax.broadcasted_iota(jnp.int32, (H, HD), 1)
    pos = lax.broadcasted_iota(jnp.int32, (1, slen), 1)
    all_m = jnp.zeros((H, HD), F32)
    all_l = jnp.zeros((H, HD), F32)
    new32 = new_ref[0].astype(F32)
    for b in range(count):
        query = qrow[pl.ds(b, H, stride=count), :]
        spread = jnp.concatenate(
            [jnp.where(row_group == g, query, 0.0) for g in range(KVH)], axis=1
        )
        own = spread * new32[b : b + 1, :KW]
        folded = own[:, :HD]
        for g in range(1, KVH):
            folded = folded + own[:, g * HD : (g + 1) * HD]
        own_score = jnp.sum(folded, axis=1, keepdims=True) * FACTOR
        suf_copies[b].wait()
        scores = lax.dot_general(
            spread.astype(BF16), suf[b, :, :KW], NT, preferred_element_type=F32
        )
        scores = jnp.where(pos < slen_ref[0, b], scores * FACTOR, NEG)
        top = jnp.maximum(jnp.max(scores, axis=1, keepdims=True), own_score)
        weights = jnp.exp2(scores - top)
        own_weight = jnp.exp2(own_score - top)
        norm = jnp.sum(weights, axis=1, keepdims=True) + own_weight
        wide = jnp.dot(
            weights.astype(BF16), suf[b, :, KW:], preferred_element_type=F32
        )
        wide = wide + own_weight.astype(BF16).astype(F32) * new32[b : b + 1, KW:]
        result = jnp.where(row_group == 0, wide[:, :HD], 0.0)
        for g in range(1, KVH):
            result = jnp.where(row_group == g, wide[:, g * HD : (g + 1) * HD], result)
        orow[pl.ds(b, H, stride=count), :] = result / norm
        all_m = jnp.where(lane == b, top, all_m)
        all_l = jnp.where(lane == b, norm, all_l)
    for h in range(H):
        half, col = h // HALF_H, (h % HALF_H) * HD
        ssrc[half, :, col : col + HD] = orow[h * count : (h + 1) * count, :].astype(BF16)
    for half in range(2):
        rows = slice(half * HALF_H, (half + 1) * HALF_H)
        block = jnp.concatenate(
            [all_m[rows], all_l[rows], jnp.zeros((HD - 2 * HALF_H, HD), F32)], axis=0
        )
        stsrc[half] = block.T[:count, :]

    def s_copy(d):
        to = (me + d) % n
        return remote(ssrc.at[to % 2], sall.at[me], s_send.at[d], s_recv.at[d], to)

    def t_copy(d):
        to = (me + d) % n
        return remote(stsrc.at[to % 2], stall.at[me], t_send.at[d], t_recv.at[d], to)

    for d in order:
        t_copy(d).start()
        s_copy(d).start()
    own_s = pltpu.make_async_copy(ssrc.at[core], sall.at[me], q_sem)
    own_t = pltpu.make_async_copy(stsrc.at[core], stall.at[me], q_sem)

    own_q.wait()
    own_s.start()
    own_s.wait()
    own_t.start()
    own_t.wait()
    for d in range(1, n):
        q_copy(d).wait_recv()

    owner = owner_ref[0]
    owner_chip = owner // 2
    slot = owner % 2
    plen = plen_ref[0]
    positions = kv0.shape[2]
    bias = jnp.where(
        lax.broadcasted_iota(jnp.int32, (1, positions), 1) < plen, 0.0, NEG
    ).astype(F32)
    wide_lane = lax.broadcasted_iota(jnp.int32, (total, HD), 1)

    last = HALF_G

    def right_copy(k):
        if isinstance(k, int) and k == last:
            src, dst = to_right_st, from_left_st
        else:
            src, dst = to_right.at[k], from_left.at[k]
        return remote(src, dst, r_send.at[k], r_recv.at[k], (me + 2) % n)

    def left_copy(k):
        if isinstance(k, int) and k == last:
            src, dst = to_left_st, from_right_st
        else:
            src, dst = to_left.at[k], from_right.at[k]
        return remote(src, dst, l_send.at[k], l_recv.at[k], (me + n - 2) % n)

    def head(k, stats):
        for part in range(2):
            kv_local(k, part).wait()
            kv_arrival(k, part).wait_recv()
        rows = [
            qall[:, :, k * GW + j * HD : k * GW + (j + 1) * HD]
            .astype(F32)
            .reshape(total, HD)
            for j in range(GROUP)
        ]
        query = jnp.concatenate(rows, axis=0).astype(BF16)
        scores = lax.dot_general(query, kv[k][slot, 0], NT, preferred_element_type=F32)
        scores = scores * FACTOR + bias
        top = jnp.max(scores, axis=1, keepdims=True)
        weights = jnp.exp2(scores - top)
        norm = jnp.sum(weights, axis=1, keepdims=True)
        result = jnp.dot(weights.astype(BF16), kv[k][slot, 1], preferred_element_type=F32)
        result = (result / norm).astype(BF16)
        block = jnp.concatenate(
            [result[j * total : (j + 1) * total] for j in range(GROUP)], axis=1
        )
        mine[k] = block
        for j in range(GROUP):
            at = k * GROUP + j
            part = slice(j * total, (j + 1) * total)
            stats = jnp.where(wide_lane == at, top[part], stats)
            stats = jnp.where(wide_lane == HALF_H + at, norm[part], stats)

        @pl.when(chip == 0)
        def _():
            to_right[k] = block
            right_copy(k).start()

        @pl.when(chip == chips - 1)
        def _():
            to_left[k] = block
            left_copy(k).start()

        return stats

    stats = jnp.zeros((total, HD), F32)
    for k in range(HALF_G):
        stats = head(k, stats)
    minest[...] = stats

    @pl.when(chip == 0)
    def _():
        to_right_st[...] = stats
        right_copy(last).start()

    @pl.when(chip == chips - 1)
    def _():
        to_left_st[...] = stats
        left_copy(last).start()

    is_mine = owner_chip == chip
    for k in range(last + 1):
        here = minest if k == last else mine.at[k]
        left_in = from_left_st if k == last else from_left.at[k]
        right_in = from_right_st if k == last else from_right.at[k]
        right_out = to_right_st if k == last else to_right.at[k]
        left_out = to_left_st if k == last else to_left.at[k]

        @pl.when(chip > 0)
        def _():
            right_copy(k).wait_recv()

        @pl.when(jnp.logical_and(chip > 0, chip < chips - 1))
        def _():
            right_out[...] = jnp.where(is_mine, here[...], left_in[...])
            right_copy(k).start()

        @pl.when(chip < chips - 1)
        def _():
            left_copy(k).wait_recv()

        @pl.when(jnp.logical_and(chip > 0, chip < chips - 1))
        def _():
            left_out[...] = jnp.where(is_mine, here[...], right_in[...])
            left_copy(k).start()

    for d in range(1, n):
        t_copy(d).wait_recv()
        s_copy(d).wait_recv()

    @pl.when(chip == 0)
    def _():
        from_left_st[...] = minest[...]
        from_left[...] = mine[...]

    @pl.when(chip == chips - 1)
    def _():
        from_right_st[...] = minest[...]
        from_right[...] = mine[...]

    before = owner_chip < chip

    def pick(own, left, right):
        return jnp.where(is_mine, own, jnp.where(before, left, right))

    pre = pick(minest[...], from_left_st[...], from_right_st[...])
    post = stall[...].reshape(total, HD)
    m_pre, l_pre = pre[:, :HALF_H], pre[:, HALF_H : 2 * HALF_H]
    m_suf, l_suf = post[:, :HALF_H], post[:, HALF_H : 2 * HALF_H]
    top = jnp.maximum(m_pre, m_suf)
    part_pre = l_pre * jnp.exp2(m_pre - top)
    part_suf = l_suf * jnp.exp2(m_suf - top)
    denom = part_pre + part_suf
    share_pre = part_pre / denom
    share_suf = part_suf / denom

    def a_copy(k):
        return remote(attn.at[k], attn_in.at[k], a_send.at[k], a_recv.at[k], partner)

    for k in range(HALF_G):
        prefix = pick(mine[k], from_left[k], from_right[k])
        for j in range(GROUP):
            h = k * GROUP + j
            cols = slice(h * HD, (h + 1) * HD)
            suffix = sall[:, :, cols].astype(F32).reshape(total, HD)
            value = (
                prefix[:, j * HD : (j + 1) * HD].astype(F32) * share_pre[:, h : h + 1]
                + suffix * share_suf[:, h : h + 1]
            )
            attn[k, :, j * HD : (j + 1) * HD] = value.astype(BF16)
        a_copy(k).start()

    for half in range(2):
        w_copy(half).wait()
    acc = jnp.zeros(out_ref.shape[1:], F32)
    for k in range(HALF_G):
        acc = acc + jnp.dot(
            attn[k], wbuf[core, k * GW : (k + 1) * GW, :], preferred_element_type=F32
        )
    for k in range(HALF_G):
        a_copy(k).wait_recv()
        acc = acc + jnp.dot(
            attn_in[k],
            wbuf[1 - core, k * GW : (k + 1) * GW, :],
            preferred_element_type=F32,
        )
    out_ref[0] = acc.astype(BF16)

    for d in range(1, n):
        q_copy(d).wait_send()
        t_copy(d).wait_send()
        s_copy(d).wait_send()
    for k in range(HALF_G):
        a_copy(k).wait_send()
        for part in range(2):
            kv_remote(k, part).wait_send()
    for k in range(last + 1):

        @pl.when(chip < chips - 1)
        def _():
            right_copy(k).wait_send()

        @pl.when(chip > 0)
        def _():
            left_copy(k).wait_send()


def local(n, queries, prompt_cache, owner, prompt_len, suffix_cache, suffix_len, new_kv, out_weight):
    count = queries.shape[1]
    total = n * count
    slen = suffix_cache.shape[2]
    positions = prompt_cache.shape[2]
    width = out_weight.shape[1]
    smem = pl.BlockSpec(memory_space=pltpu.SMEM)
    vmem = pl.BlockSpec(memory_space=pltpu.VMEM)
    hbm = pl.BlockSpec(memory_space=pltpu.HBM)
    dma = pltpu.SemaphoreType.DMA
    chunk = pltpu.VMEM((HALF_G, total, GW), BF16)
    stat = pltpu.VMEM((total, HD), F32)
    return pl.pallas_call(
        functools.partial(kernel, n),
        out_shape=jax.ShapeDtypeStruct((1, total, width), BF16),
        in_specs=[smem, smem, smem, vmem, vmem, hbm, hbm, hbm],
        out_specs=vmem,
        scratch_shapes=[
            *[pltpu.VMEM((2, 2, positions, HD), BF16)] * HALF_G,
            pltpu.VMEM((count, slen, 2 * KW), BF16),
            pltpu.VMEM((2, HALF_W, width), BF16),
            pltpu.VMEM((2, count, HALF_W), BF16),
            pltpu.VMEM((n, count, HALF_W), BF16),
            pltpu.VMEM((H * count, HD), F32),
            pltpu.VMEM((H * count, HD), F32),
            pltpu.VMEM((2, count, HALF_W), BF16),
            pltpu.VMEM((n, count, HALF_W), BF16),
            pltpu.VMEM((2, count, HD), F32),
            pltpu.VMEM((n, count, HD), F32),
            chunk,
            stat,
            chunk,
            stat,
            chunk,
            stat,
            chunk,
            stat,
            chunk,
            stat,
            chunk,
            chunk,
            dma((count,)),
            dma((HALF_G, 2)),
            dma((2,)),
            dma(()),
            dma((n,)),
            dma((n,)),
            dma((n,)),
            dma((n,)),
            dma((n,)),
            dma((n,)),
            dma((HALF_G, 2)),
            dma((HALF_G, 2)),
            dma((HALF_G + 1,)),
            dma((HALF_G + 1,)),
            dma((HALF_G + 1,)),
            dma((HALF_G + 1,)),
            dma((HALF_G,)),
            dma((HALF_G,)),
        ],
        compiler_params=pltpu.CompilerParams(
            collective_id=0, has_side_effects=True, vmem_limit_bytes=60 * 1024 * 1024
        ),
        name="shared_decode",
    )(owner, prompt_len, suffix_len, queries, new_kv, prompt_cache, suffix_cache, out_weight)


def solution(mesh):
    in_specs = (
        P("prompt", "sample", None),
        P("prompt", "sample", None, None),
        P("prompt"),
        P("prompt"),
        P("prompt", "sample", None, None),
        P("prompt", "sample"),
        P("prompt", "sample", None),
        P(None, "sample"),
    )
    out_specs = P("prompt", None, "sample")
    body = functools.partial(local, mesh.shape["sample"])
    return jax.shard_map(body, mesh=mesh, in_specs=in_specs, out_specs=out_specs, check_vma=False)
```

```python
import functools

import jax
import jax.numpy as jnp
from jax import lax
from jax.experimental import pallas as pl
from jax.experimental.pallas import tpu as pltpu
from jax.sharding import PartitionSpec as P

H = 32
KVH = 8
HD = 128
GROUP = H // KVH
HALF_H = H // 2
HALF_G = KVH // 2
HALF_W = HALF_H * HD
KW = KVH * HD
GW = GROUP * HD
FACTOR = HD ** (-0.5) * 1.4426950408889634
NEG = -1e30
HOP = 2.4
F32 = jnp.float32
BF16 = jnp.bfloat16
NT = (((1,), (1,)), ((), ()))


def kernel(
    n,
    owner_ref,
    plen_ref,
    slen_ref,
    q_ref,
    new_ref,
    cache_ref,
    suffix_ref,
    w_ref,
    out_ref,
    kv0,
    kv1,
    kv2,
    kv3,
    suf,
    wbuf,
    qsrc,
    qall,
    qrow,
    orow,
    ssrc,
    sall,
    stsrc,
    stall,
    mine,
    minest,
    from_left,
    from_left_st,
    from_right,
    from_right_st,
    to_right,
    to_right_st,
    to_left,
    to_left_st,
    attn,
    attn_in,
    suf_sem,
    kv_sem,
    w_sem,
    q_sem,
    q_send,
    q_recv,
    s_send,
    s_recv,
    t_send,
    t_recv,
    kv_send,
    kv_recv,
    r_send,
    r_recv,
    l_send,
    l_recv,
    a_send,
    a_recv,
):
    kv = (kv0, kv1, kv2, kv3)
    me = lax.axis_index("sample")
    chip = me // 2
    core = me % 2
    chips = n // 2
    partner = chip * 2 + (1 - core)
    count = q_ref.shape[1]
    total = n * count
    slen = suffix_ref.shape[2]

    def remote(src, dst, send, recv, to):
        return pltpu.make_async_remote_copy(
            src_ref=src,
            dst_ref=dst,
            send_sem=send,
            recv_sem=recv,
            device_id={"sample": to},
            device_id_type=pl.DeviceIdType.MESH,
        )

    suf_copies = [
        pltpu.make_async_copy(suffix_ref.at[0, b], suf.at[b], suf_sem.at[b])
        for b in range(count)
    ]
    for copy in suf_copies:
        copy.start()

    barrier = pltpu.get_barrier_semaphore()
    for d in range(1, n):
        pl.semaphore_signal(
            barrier,
            inc=1,
            device_id={"sample": (me + d) % n},
            device_id_type=pl.DeviceIdType.MESH,
        )

    q32 = q_ref[0].astype(F32)
    for half in range(2):
        qsrc[half] = q_ref[0, :, half * HALF_W : (half + 1) * HALF_W]
    for h in range(H):
        qrow[h * count : (h + 1) * count, :] = q32[:, h * HD : (h + 1) * HD]

    def kv_local(k, part):
        col = part * KW + (core * HALF_G + k) * HD
        return pltpu.make_async_copy(
            cache_ref.at[0, 0, :, pl.ds(pl.multiple_of(col, HD), HD)],
            kv[k].at[core, part],
            kv_sem.at[k, part],
        )

    def kv_remote(k, part):
        col = part * KW + ((1 - core) * HALF_G + k) * HD
        return remote(
            cache_ref.at[0, 0, :, pl.ds(pl.multiple_of(col, HD), HD)],
            kv[k].at[core, part],
            kv_send.at[k, part],
            kv_recv.at[k, part],
            partner,
        )

    def kv_arrival(k, part):
        return remote(
            kv[k].at[1 - core, part],
            kv[k].at[1 - core, part],
            kv_send.at[k, part],
            kv_recv.at[k, part],
            partner,
        )

    def w_copy(half):
        return pltpu.make_async_copy(
            w_ref.at[pl.ds(half * HALF_W, HALF_W), :], wbuf.at[half], w_sem.at[half]
        )

    pl.semaphore_wait(barrier, n - 1)

    def q_copy(d):
        to = (me + d) % n
        return remote(qsrc.at[to % 2], qall.at[me], q_send.at[d], q_recv.at[d], to)

    order = sorted(range(1, n), key=lambda d: -min(d, n - d))
    for d in order:
        q_copy(d).start()
    own_q = pltpu.make_async_copy(qsrc.at[core], qall.at[me], q_sem)
    own_q.start()
    for k in range(HALF_G):
        for part in range(2):
            kv_remote(k, part).start()
    for k in range(HALF_G):
        for part in range(2):
            kv_local(k, part).start()
    for half in range(2):
        w_copy(half).start()

    row_group = lax.broadcasted_iota(jnp.int32, (H, HD), 0) // GROUP
    lane = lax.broadcasted_iota(jnp.int32, (H, HD), 1)
    pos = lax.broadcasted_iota(jnp.int32, (1, slen), 1)
    all_m = jnp.zeros((H, HD), F32)
    all_l = jnp.zeros((H, HD), F32)
    new32 = new_ref[0].astype(F32)
    for b in range(count):
        query = qrow[pl.ds(b, H, stride=count), :]
        spread = jnp.concatenate(
            [jnp.where(row_group == g, query, 0.0) for g in range(KVH)], axis=1
        )
        own = spread * new32[b : b + 1, :KW]
        folded = own[:, :HD]
        for g in range(1, KVH):
            folded = folded + own[:, g * HD : (g + 1) * HD]
        own_score = jnp.sum(folded, axis=1, keepdims=True) * FACTOR
        suf_copies[b].wait()
        scores = lax.dot_general(
            spread.astype(BF16), suf[b, :, :KW], NT, preferred_element_type=F32
        )
        scores = jnp.where(pos < slen_ref[0, b], scores * FACTOR, NEG)
        top = jnp.maximum(jnp.max(scores, axis=1, keepdims=True), own_score)
        weights = jnp.exp2(scores - top)
        own_weight = jnp.exp2(own_score - top)
        norm = jnp.sum(weights, axis=1, keepdims=True) + own_weight
        wide = jnp.dot(
            weights.astype(BF16), suf[b, :, KW:], preferred_element_type=F32
        )
        wide = wide + own_weight.astype(BF16).astype(F32) * new32[b : b + 1, KW:]
        result = jnp.where(row_group == 0, wide[:, :HD], 0.0)
        for g in range(1, KVH):
            result = jnp.where(row_group == g, wide[:, g * HD : (g + 1) * HD], result)
        orow[pl.ds(b, H, stride=count), :] = result / norm
        all_m = jnp.where(lane == b, top, all_m)
        all_l = jnp.where(lane == b, norm, all_l)
    for h in range(H):
        half, col = h // HALF_H, (h % HALF_H) * HD
        ssrc[half, :, col : col + HD] = orow[h * count : (h + 1) * count, :].astype(BF16)
    for half in range(2):
        rows = slice(half * HALF_H, (half + 1) * HALF_H)
        block = jnp.concatenate(
            [all_m[rows], all_l[rows], jnp.zeros((HD - 2 * HALF_H, HD), F32)], axis=0
        )
        stsrc[half] = block.T[:count, :]

    def s_copy(d):
        to = (me + d) % n
        return remote(ssrc.at[to % 2], sall.at[me], s_send.at[d], s_recv.at[d], to)

    def t_copy(d):
        to = (me + d) % n
        return remote(stsrc.at[to % 2], stall.at[me], t_send.at[d], t_recv.at[d], to)

    for d in order:
        t_copy(d).start()
        s_copy(d).start()
    own_s = pltpu.make_async_copy(ssrc.at[core], sall.at[me], q_sem)
    own_t = pltpu.make_async_copy(stsrc.at[core], stall.at[me], q_sem)

    own_q.wait()
    own_s.start()
    own_s.wait()
    own_t.start()
    own_t.wait()
    for d in range(1, n):
        q_copy(d).wait_recv()

    owner = owner_ref[0]
    owner_chip = owner // 2
    slot = owner % 2
    plen = plen_ref[0]
    positions = kv0.shape[2]
    bias = jnp.where(
        lax.broadcasted_iota(jnp.int32, (1, positions), 1) < plen, 0.0, NEG
    ).astype(F32)
    wide_lane = lax.broadcasted_iota(jnp.int32, (total, HD), 1)

    last = HALF_G

    def right_copy(k):
        if isinstance(k, int) and k == last:
            src, dst = to_right_st, from_left_st
        else:
            src, dst = to_right.at[k], from_left.at[k]
        return remote(src, dst, r_send.at[k], r_recv.at[k], (me + 2) % n)

    def left_copy(k):
        if isinstance(k, int) and k == last:
            src, dst = to_left_st, from_right_st
        else:
            src, dst = to_left.at[k], from_right.at[k]
        return remote(src, dst, l_send.at[k], l_recv.at[k], (me + n - 2) % n)

    def head(k, stats):
        for part in range(2):
            kv_local(k, part).wait()
            kv_arrival(k, part).wait_recv()
        rows = [
            qall[:, :, k * GW + j * HD : k * GW + (j + 1) * HD]
            .astype(F32)
            .reshape(total, HD)
            for j in range(GROUP)
        ]
        query = jnp.concatenate(rows, axis=0).astype(BF16)
        scores = lax.dot_general(query, kv[k][slot, 0], NT, preferred_element_type=F32)
        scores = scores * FACTOR + bias
        top = jnp.max(scores, axis=1, keepdims=True)
        weights = jnp.exp2(scores - top)
        norm = jnp.sum(weights, axis=1, keepdims=True)
        result = jnp.dot(weights.astype(BF16), kv[k][slot, 1], preferred_element_type=F32)
        result = (result / norm).astype(BF16)
        block = jnp.concatenate(
            [result[j * total : (j + 1) * total] for j in range(GROUP)], axis=1
        )
        mine[k] = block
        for j in range(GROUP):
            at = k * GROUP + j
            part = slice(j * total, (j + 1) * total)
            stats = jnp.where(wide_lane == at, top[part], stats)
            stats = jnp.where(wide_lane == HALF_H + at, norm[part], stats)

        @pl.when(chip == 0)
        def _():
            to_right[k] = block
            right_copy(k).start()

        @pl.when(chip == chips - 1)
        def _():
            to_left[k] = block
            left_copy(k).start()

        return stats

    stats = jnp.zeros((total, HD), F32)
    for k in range(HALF_G):
        stats = head(k, stats)
    minest[...] = stats

    @pl.when(chip == 0)
    def _():
        to_right_st[...] = stats
        right_copy(last).start()

    @pl.when(chip == chips - 1)
    def _():
        to_left_st[...] = stats
        left_copy(last).start()

    is_mine = owner_chip == chip
    def relay_right(k, forward):
        right_copy(k).wait_recv()
        if forward:
            if k == last:
                here, came, out = minest, from_left_st, to_right_st
            else:
                here, came, out = mine.at[k], from_left.at[k], to_right.at[k]
            out[...] = jnp.where(is_mine, here[...], came[...])
            right_copy(k).start()

    def relay_left(k, forward):
        left_copy(k).wait_recv()
        if forward:
            if k == last:
                here, came, out = minest, from_right_st, to_left_st
            else:
                here, came, out = mine.at[k], from_right.at[k], to_left.at[k]
            out[...] = jnp.where(is_mine, here[...], came[...])
            left_copy(k).start()

    for z in range(chips):

        @pl.when(chip == z)
        def _():
            steps = []
            for k in range(last + 1):
                if z > 0:
                    steps.append((z * HOP + k, k, relay_right, z < chips - 1))
                if z < chips - 1:
                    steps.append(((chips - 1 - z) * HOP + k, k, relay_left, z > 0))
            for _, k, relay, forward in sorted(steps, key=lambda step: step[0]):
                relay(k, forward)

    for d in range(1, n):
        t_copy(d).wait_recv()
        s_copy(d).wait_recv()

    @pl.when(chip == 0)
    def _():
        from_left_st[...] = minest[...]
        from_left[...] = mine[...]

    @pl.when(chip == chips - 1)
    def _():
        from_right_st[...] = minest[...]
        from_right[...] = mine[...]

    before = owner_chip < chip

    def pick(own, left, right):
        return jnp.where(is_mine, own, jnp.where(before, left, right))

    pre = pick(minest[...], from_left_st[...], from_right_st[...])
    post = stall[...].reshape(total, HD)
    m_pre, l_pre = pre[:, :HALF_H], pre[:, HALF_H : 2 * HALF_H]
    m_suf, l_suf = post[:, :HALF_H], post[:, HALF_H : 2 * HALF_H]
    top = jnp.maximum(m_pre, m_suf)
    part_pre = l_pre * jnp.exp2(m_pre - top)
    part_suf = l_suf * jnp.exp2(m_suf - top)
    denom = part_pre + part_suf
    share_pre = part_pre / denom
    share_suf = part_suf / denom

    def a_copy(k):
        return remote(attn.at[k], attn_in.at[k], a_send.at[k], a_recv.at[k], partner)

    for k in range(HALF_G):
        prefix = pick(mine[k], from_left[k], from_right[k])
        for j in range(GROUP):
            h = k * GROUP + j
            cols = slice(h * HD, (h + 1) * HD)
            suffix = sall[:, :, cols].astype(F32).reshape(total, HD)
            value = (
                prefix[:, j * HD : (j + 1) * HD].astype(F32) * share_pre[:, h : h + 1]
                + suffix * share_suf[:, h : h + 1]
            )
            attn[k, :, j * HD : (j + 1) * HD] = value.astype(BF16)
        a_copy(k).start()

    for half in range(2):
        w_copy(half).wait()
    acc = jnp.zeros(out_ref.shape[1:], F32)
    for k in range(HALF_G):
        acc = acc + jnp.dot(
            attn[k], wbuf[core, k * GW : (k + 1) * GW, :], preferred_element_type=F32
        )
    for k in range(HALF_G):
        a_copy(k).wait_recv()
        acc = acc + jnp.dot(
            attn_in[k],
            wbuf[1 - core, k * GW : (k + 1) * GW, :],
            preferred_element_type=F32,
        )
    out_ref[0] = acc.astype(BF16)

    for d in range(1, n):
        q_copy(d).wait_send()
        t_copy(d).wait_send()
        s_copy(d).wait_send()
    for k in range(HALF_G):
        a_copy(k).wait_send()
        for part in range(2):
            kv_remote(k, part).wait_send()
    for k in range(last + 1):

        @pl.when(chip < chips - 1)
        def _():
            right_copy(k).wait_send()

        @pl.when(chip > 0)
        def _():
            left_copy(k).wait_send()


def local(n, queries, prompt_cache, owner, prompt_len, suffix_cache, suffix_len, new_kv, out_weight):
    count = queries.shape[1]
    total = n * count
    slen = suffix_cache.shape[2]
    positions = prompt_cache.shape[2]
    width = out_weight.shape[1]
    smem = pl.BlockSpec(memory_space=pltpu.SMEM)
    vmem = pl.BlockSpec(memory_space=pltpu.VMEM)
    hbm = pl.BlockSpec(memory_space=pltpu.HBM)
    dma = pltpu.SemaphoreType.DMA
    chunk = pltpu.VMEM((HALF_G, total, GW), BF16)
    stat = pltpu.VMEM((total, HD), F32)
    return pl.pallas_call(
        functools.partial(kernel, n),
        out_shape=jax.ShapeDtypeStruct((1, total, width), BF16),
        in_specs=[smem, smem, smem, vmem, vmem, hbm, hbm, hbm],
        out_specs=vmem,
        scratch_shapes=[
            *[pltpu.VMEM((2, 2, positions, HD), BF16)] * HALF_G,
            pltpu.VMEM((count, slen, 2 * KW), BF16),
            pltpu.VMEM((2, HALF_W, width), BF16),
            pltpu.VMEM((2, count, HALF_W), BF16),
            pltpu.VMEM((n, count, HALF_W), BF16),
            pltpu.VMEM((H * count, HD), F32),
            pltpu.VMEM((H * count, HD), F32),
            pltpu.VMEM((2, count, HALF_W), BF16),
            pltpu.VMEM((n, count, HALF_W), BF16),
            pltpu.VMEM((2, count, HD), F32),
            pltpu.VMEM((n, count, HD), F32),
            chunk,
            stat,
            chunk,
            stat,
            chunk,
            stat,
            chunk,
            stat,
            chunk,
            stat,
            chunk,
            chunk,
            dma((count,)),
            dma((HALF_G, 2)),
            dma((2,)),
            dma(()),
            dma((n,)),
            dma((n,)),
            dma((n,)),
            dma((n,)),
            dma((n,)),
            dma((n,)),
            dma((HALF_G, 2)),
            dma((HALF_G, 2)),
            dma((HALF_G + 1,)),
            dma((HALF_G + 1,)),
            dma((HALF_G + 1,)),
            dma((HALF_G + 1,)),
            dma((HALF_G,)),
            dma((HALF_G,)),
        ],
        compiler_params=pltpu.CompilerParams(
            collective_id=0, has_side_effects=True, vmem_limit_bytes=60 * 1024 * 1024
        ),
        name="shared_decode",
    )(owner, prompt_len, suffix_len, queries, new_kv, prompt_cache, suffix_cache, out_weight)


def solution(mesh):
    in_specs = (
        P("prompt", "sample", None),
        P("prompt", "sample", None, None),
        P("prompt"),
        P("prompt"),
        P("prompt", "sample", None, None),
        P("prompt", "sample"),
        P("prompt", "sample", None),
        P(None, "sample"),
    )
    out_specs = P("prompt", None, "sample")
    body = functools.partial(local, mesh.shape["sample"])
    return jax.shard_map(body, mesh=mesh, in_specs=in_specs, out_specs=out_specs, check_vma=False)
```
